32 devices in a mesh: bra: 8 (over z, x), ket: 2 (over y), mpo: 2 (over core).
Axes of the slice: x: 2, y: 2, z: 4, core: 2. Of those that a mesh axis runs over, the one named last changes fastest.
Arguments:
- left_env: bfloat16 [4, 3072, 3072], P('mpo', 'bra', 'ket'), may hold values from -6 to 6
- site_tensor: bfloat16 [3072, 4, 3072], P('bra', None, 'ket'), may hold values from -0.0546875 to 0.0546875
- block_values: float32 [12, 4, 4], replicated, may hold values from -3 to 3
- pair_in: int32 [12], replicated, may hold values from 0 to 3
- pair_out: int32 [12], replicated, may hold values from 0 to 3, as said below
Outputs:
- new_env: bfloat16 [4, 3072, 3072], P('mpo', 'bra', 'ket')
The draws below stay inside these ranges and needn't reach their ends.
Inputs may be any that keep to these rules, and one draw needn't show every extreme that they name: `pair_out`: every component number 0 to 3 appears at least once.
All inputs are finite; a program needn't handle non-finite values.
Results may differ from the reference program's by a relative error of at most 0.018.
Values may be sent and summed in bfloat16 or wider, within the bound.
A program may use at most 192 MiB of HBM per device.

```python
import jax
import jax.numpy as jnp
from jax import lax

D = 3072
PHYS = 4
K = 4
NNZ = 12
N_BRA = 8


def draw_pair_out(key, part):
    first = jax.random.permutation(jax.random.fold_in(key, 11), K).astype(jnp.int32)
    extra = jax.random.randint(jax.random.fold_in(key, 12), (NNZ - K,), 0, K).astype(jnp.int32)
    return jnp.concatenate([first, extra]).astype(jnp.int32)


def touch_ends(result, own_key, smallest, high):
    extent = result.shape
    spot = [jax.random.randint(jax.random.fold_in(own_key, axis), (), 0, extent[axis]) for axis in range(len(extent))]
    result = result.at[tuple(spot)].set(smallest)
    longest = extent.index(max(extent))
    spot[longest] = (spot[longest] + 1) % extent[longest]
    return result.at[tuple(spot)].set(high)


def steps_of(rng, dims, split, smallest, top_value):
    def one(dim, parts):
        steps = jax.random.uniform(jax.random.fold_in(jax.random.fold_in(rng, 6), dim), (parts,), jnp.float32, smallest / len(split), top_value / len(split))
        return jnp.repeat(jnp.exp(steps), dims[dim] // parts).reshape((-1,) + (1,) * (len(dims) - dim - 1))

    factor_of = one(*split[0])
    for cut in split[1:]:
        factor_of = factor_of * one(*cut)
    return factor_of


def bell_draw(rng, extent, width, bound, pieces=(), held_as=jnp.bfloat16):
    entries = width * jax.random.normal(rng, extent, jnp.float32)
    if pieces:
        entries = entries * steps_of(rng, extent, pieces, -0.22, 0.18)
    return jnp.clip(entries, -bound, bound).astype(held_as)


def setup_inputs(seed: int = 0) -> dict:
    streams_of = jax.random.split(jax.random.key(seed), 6)
    left_env = bell_draw(streams_of[0], (K, D, D), 1.0, 6.0, ((0, 2), (1, 8), (2, 2)))
    site_tensor = bell_draw(streams_of[1], (D, PHYS, D), (PHYS * D) ** -0.5, 0.0546875, ((0, 8), (2, 2)))
    block_values = bell_draw(streams_of[2], (NNZ, PHYS, PHYS), 0.5, 3.0, (), jnp.float32)
    pair_in = touch_ends(jax.random.randint(streams_of[3], (NNZ,), 0, K), jax.random.fold_in(streams_of[3], 1), 0, K - 1).astype(jnp.int32)
    pair_out = draw_pair_out(jax.random.fold_in(streams_of[5], 71), 0)
    return {"left_env": left_env, "site_tensor": site_tensor, "block_values": block_values, "pair_in": pair_in, "pair_out": pair_out}


def reference(left_env, site_tensor, block_values, pair_in, pair_out):
    comps = jnp.arange(K, dtype=jnp.int32)
    hot_out = (pair_out[:, None] == comps[None, :]).astype(jnp.float32)
    hot_in = (pair_in[:, None] == comps[None, :]).astype(jnp.float32)
    mixing = jnp.einsum("pv,pw,pst->vswt", hot_out, hot_in, block_values, precision=lax.Precision.HIGHEST)
    flat_site = site_tensor.reshape(D, PHYS * D)

    def one_comp(env):
        return jnp.dot(env, flat_site, preferred_element_type=jnp.float32).astype(jnp.bfloat16)

    half = lax.map(one_comp, left_env).reshape(K, D, PHYS, D)
    mixed = jnp.einsum("vswt,watc->vasc", mixing, half.astype(jnp.float32), precision=lax.Precision.HIGHEST).astype(jnp.bfloat16)
    rows_blk = D // N_BRA

    def add_block(index, total):
        start = (index * rows_blk).astype(jnp.int32)
        site_blk = lax.dynamic_slice_in_dim(site_tensor, start, rows_blk, 0).reshape(rows_blk * PHYS, D)
        mixed_blk = lax.dynamic_slice_in_dim(mixed, start, rows_blk, 1).reshape(K, rows_blk * PHYS, D)
        term = jnp.einsum("ke,wkc->wec", site_blk.astype(jnp.float32), mixed_blk.astype(jnp.float32))
        return total + term.astype(jnp.bfloat16).astype(jnp.float32)

    total = lax.fori_loop(0, N_BRA, add_block, jnp.zeros((K, D, D), jnp.float32))
    return total.astype(jnp.bfloat16)
```

```python
import functools

import jax
import jax.numpy as jnp
from jax import lax
from jax.experimental import pallas as pl
from jax.experimental.pallas import tpu as pltpu
from jax.sharding import PartitionSpec as P

K = 4
LANES = 128
MESH = pl.DeviceIdType.MESH
BF16 = jnp.bfloat16
F32 = jnp.float32


def mixing_of(block_values, pair_in, pair_out):
    comps = jnp.arange(K, dtype=jnp.int32)
    hot_out = (pair_out[:, None] == comps[None, :]).astype(F32)
    hot_in = (pair_in[:, None] == comps[None, :]).astype(F32)
    return jnp.einsum(
        "pv,pw,pst->vswt", hot_out, hot_in, block_values, precision=lax.Precision.HIGHEST
    )


def plain(left_env, site_tensor, block_values, pair_in, pair_out):
    rows_loc = left_env.shape[1]
    cols_loc = left_env.shape[2]
    phys = site_tensor.shape[1]
    mixing = mixing_of(block_values, pair_in, pair_out)
    splits = lax.axis_size("mpo")
    half_cols = cols_loc // splits
    own_start = lax.axis_index("mpo") * half_cols
    site_own = lax.dynamic_slice_in_dim(site_tensor, own_start, half_cols, 2)
    site_full = lax.all_gather(
        site_own.reshape(rows_loc, phys * half_cols), "bra", axis=0, tiled=True
    )
    piece = lax.all_gather(left_env, "ket", axis=2, tiled=True)
    piece = lax.all_gather(piece, "mpo", axis=0, tiled=True)
    comps_all, width = piece.shape[0], piece.shape[2]
    half = jnp.dot(
        piece.reshape(comps_all * rows_loc, width), site_full, preferred_element_type=F32
    )
    half = half.astype(BF16).reshape(comps_all, rows_loc, phys, half_cols)
    mixed = jnp.einsum(
        "vswt,watc->savc", mixing, half.astype(F32), precision=lax.Precision.HIGHEST
    ).astype(BF16)
    mixed_pairs = mixed.reshape(phys * rows_loc, comps_all * half_cols)
    site_wide = lax.all_gather(
        jnp.transpose(site_tensor, (1, 0, 2)), "ket", axis=2, tiled=True
    )
    site_pairs = site_wide.reshape(phys * rows_loc, site_wide.shape[2])
    term = lax.dot_general(
        site_pairs, mixed_pairs, (((0,), (0,)), ((), ())), preferred_element_type=F32
    ).astype(BF16)
    owned = lax.psum_scatter(term, "bra", scatter_dimension=0, tiled=True)
    owned = jnp.transpose(owned.reshape(-1, comps_all, half_cols), (1, 0, 2))
    return lax.all_to_all(owned, "mpo", split_axis=0, concat_axis=2, tiled=True)


def update_kernel(
    nz, nj, rows, phys,
    l_ref, a_ref, c_ref, mk_ref,
    out_ref, up_ref, down_ref,
    env, conj, cols, half, terms, stage, total,
    own_sem, xy_send, xy_recv, col_send, col_recv, z_send, z_recv,
    up_send, up_recv, down_send, down_recv, stage_sem, fin_send, fin_recv, fin_own,
):
    bra, y, k = lax.axis_index("bra"), lax.axis_index("ket"), lax.axis_index("mpo")
    z, x = bra // 2, lax.rem(bra, 2)
    xo, yo, ko = 1 - x, 1 - y, 1 - k
    xn, yn, kn = (z * 2 + xo, y, k), (bra, yo, k), (bra, y, ko)
    xkn = (z * 2 + xo, y, ko)
    zu, zd = (bra + 2, y, k), (bra - 2, y, k)
    has_up, has_down = z < nz - 1, z > 0
    width = phys * LANES
    part = rows // 2

    barrier = pltpu.get_barrier_semaphore()
    for device in (xn, yn, kn, xkn):
        pl.semaphore_signal(barrier, inc=1, device_id=device, device_id_type=MESH)

    @pl.when(has_up)
    def _():
        pl.semaphore_signal(barrier, inc=1, device_id=zu, device_id_type=MESH)

    @pl.when(has_down)
    def _():
        pl.semaphore_signal(barrier, inc=1, device_id=zd, device_id_type=MESH)

    pl.semaphore_wait(barrier, 4 + (z + nz - 1) // nz + (2 * nz - 2 - z) // nz)

    def remote(src, dst, send, recv, device):
        return pltpu.make_async_remote_copy(
            src_ref=src, dst_ref=dst, send_sem=send, recv_sem=recv,
            device_id=device, device_id_type=MESH,
        )

    def slot(q, xs, ys, ks, h):
        if q == 0:
            return env.at[ys, xs, ks, h]
        return conj.at[2 * ys + lax.rem(h + ys, 2), xs, ks]

    def own(q, h):
        return l_ref.at[h] if q == 0 else a_ref.at[lax.rem(h + y, 2), k]

    upper, lower = pl.ds(0, part), pl.ds(part, part)

    def xy(q, h, t, receiving):
        ks = ko if receiving else k
        if t == 0:
            dst = slot(q, xo if receiving else x, y, k, h)
            src, device = own(q, h), xn
        elif t == 1:
            dst = slot(q, x, yo if receiving else y, k, h)
            src, device = own(q, h), yn
        elif t == 2:
            dst = slot(q, xo if receiving else x, yo, k, h).at[lower]
            src, device = dst, xn
        elif t == 3:
            dst = slot(q, xo, yo if receiving else y, k, h).at[upper]
            src, device = dst, yn
        else:
            dst = slot(q, xo if t in (5, 7) else x, yo if t in (6, 7) else y, ks, h)
            src, device = own(q, h) if t == 4 else dst, kn
        if receiving:
            src = dst
        return remote(src, dst, xy_send.at[q, h, t], xy_recv.at[q, h, t], device)

    def xy_start(q, h, t):
        xy(q, h, t, False).start()

    def xy_wait(q, h, t):
        xy(q, h, t, True).wait_recv()

    def from_x(q, h):
        xy_wait(q, h, 0)
        xy_start(q, h, 3)
        xy_start(q, h, 5)

    def from_y(q, h):
        xy_wait(q, h, 1)
        xy_start(q, h, 2)
        xy_start(q, h, 6)

    def diagonal(q, h):
        xy_wait(q, h, 2)
        xy_wait(q, h, 3)
        xy_start(q, h, 7)

    def from_core(q, h):
        for t in range(4 if q == 0 else 5, 8):
            xy_wait(q, h, t)

    def col_rows(index, count):
        return pl.ds(pl.multiple_of(index * rows, rows), count * rows)

    def col(j, receiving):
        dst = cols.at[j, col_rows(z * 2 + (xo if receiving else x), 1)]
        return remote(c_ref.at[xo, k, j], dst, col_send.at[j], col_recv.at[j], xn)

    def hop(j, up, s, receiving):
        piece = (z - s if receiving else z - s + 1) if up else (z + s if receiving else z + s - 1)
        ref = cols.at[j, col_rows(piece * 2, 2)]
        way = 0 if up else 1
        return remote(
            ref, ref, z_send.at[j, way, s - 1], z_recv.at[j, way, s - 1], zu if up else zd
        )

    def hop_sends(up, s):
        return (has_up & (z >= s - 1)) if up else (has_down & (z <= nz - s))

    def hop_start(j, s):
        for up in (True, False):
            @pl.when(hop_sends(up, s))
            def _():
                hop(j, up, s, False).start()

    def hop_sent(j):
        for s in range(1, nz):
            for up in (True, False):
                @pl.when(hop_sends(up, s))
                def _():
                    hop(j, up, s, False).wait_send()

    def hop_pass(j, s):
        for up in (True, False):
            @pl.when((z >= s) if up else (z < nz - s))
            def _():
                hop(j, up, s, True).wait_recv()

            if s < nz - 1:
                @pl.when(hop_sends(up, s + 1))
                def _():
                    hop(j, up, s + 1, False).start()

    deep = nz * rows

    def first_product(j):
        def body(i, carry):
            xs, ks = i // 2, lax.rem(i, 2)
            acc = jnp.dot(
                env[0, xs, ks].reshape(2 * rows, deep), cols[j, :deep], preferred_element_type=F32
            )
            acc += jnp.dot(
                env[1, xs, ks].reshape(2 * rows, deep), cols[j, deep:], preferred_element_type=F32
            )
            half[xs, pl.ds(2 * ks, 2)] = acc.astype(BF16).reshape(2, rows, width)
            return carry

        lax.fori_loop(0, 4, body, 0)

    group = 4
    span = group * 16

    def mix(j):
        per_x = rows // span

        def body(i, carry):
            xs, base = i // per_x, pl.multiple_of(lax.rem(i, per_x) * span, span)
            tiles = [
                half[xs, w, pl.ds(base, span), t * LANES:(t + 1) * LANES]
                for w in range(K) for t in range(phys)
            ]
            right = jnp.concatenate(
                [
                    jnp.concatenate([tile[g * 16:(g + 1) * 16] for tile in tiles], axis=0)
                    for g in range(group)
                ],
                axis=1,
            )
            both = jnp.dot(mk_ref[...], right, preferred_element_type=F32)
            size = K * phys * 16
            result = (both[:size] + both[size:]).astype(BF16)
            for v in range(K):
                for s in range(phys):
                    row = (v * phys + s) * 16
                    for g in range(group):
                        at = pl.multiple_of(xs * deep + s * rows + base + g * 16, 16)
                        cols[j, pl.ds(at, 16), v * LANES:(v + 1) * LANES] = result[
                            row:row + 16, g * LANES:(g + 1) * LANES
                        ]
            return carry

        lax.fori_loop(0, 2 * per_x, body, 0)

    def term_ref(j, d):
        if j < 2:
            return terms.at[j, d]
        return env.at[d // 2, d % 2, 0, :, :, pl.ds((j - 2) * width, width)]

    def up_copy(j, d):
        return remote(term_ref(j, d), up_ref.at[j, d], up_send.at[j, d], up_recv.at[j, d], zu)

    def down_copy(j, d):
        return remote(
            term_ref(j, d), down_ref.at[j, d], down_send.at[j, d], down_recv.at[j, d], zd
        )

    def second_product(j, d):
        out = term_ref(j, d)
        acc = jnp.dot(
            conj[d, 0].reshape(2 * rows, deep), cols[j, :deep], preferred_element_type=F32
        )
        acc += jnp.dot(
            conj[d, 1].reshape(2 * rows, deep), cols[j, deep:], preferred_element_type=F32
        )
        out[...] = acc.astype(BF16).reshape(2, rows, width)
        if d > 0:
            @pl.when(z == 0)
            def _():
                up_copy(j, d).start()
        if d < nz - 1:
            @pl.when(z == nz - 1)
            def _():
                down_copy(j, d).start()

    strip = 96
    strips = rows // strip

    def strip_of(i):
        return i // strips, pl.ds(pl.multiple_of(lax.rem(i, strips) * strip, strip), strip)

    def fetch(src, index):
        return pltpu.make_async_copy(src, stage.at[index], stage_sem.at[index])

    def pass_on(j, d, up):
        copy = up_copy(j, d) if up else down_copy(j, d)
        copy.wait_recv()
        local = fetch((up_ref if up else down_ref).at[j, d], 0)
        local.start()
        local.wait()
        ref = term_ref(j, d)

        def body(i, carry):
            b, r = strip_of(i)
            ref[b, r] = (ref[b, r].astype(F32) + stage[0, b, r].astype(F32)).astype(BF16)
            return carry

        lax.fori_loop(0, 2 * strips, body, 0)
        copy.start()

    def fin(j, t, receiving):
        xs, ks, device = ((x, ko, kn), (xo, k, xn), (xo, ko, xkn))[t]
        block = (xs * 2 + ks) if receiving else (x * 2 + k)
        dst = out_ref.at[
            :, :, pl.ds(pl.multiple_of((block * nj + j) * LANES, LANES), LANES)
        ]
        src = total.at[j, pl.ds(2 * ks, 2), pl.ds(pl.multiple_of(xs * rows, rows), rows)]
        return remote(src, dst, fin_send.at[j, t], fin_recv.at[j, t], device)

    def fin_local(j):
        dst = out_ref.at[
            :, :, pl.ds(pl.multiple_of(((x * 2 + k) * nj + j) * LANES, LANES), LANES)
        ]
        src = total.at[j, pl.ds(2 * k, 2), pl.ds(pl.multiple_of(x * rows, rows), rows)]
        return pltpu.make_async_copy(src, dst, fin_own.at[j])

    def finish(j, d):
        below, above = d > 0, d < nz - 1
        count = 0
        for there, copy, src in ((below, up_copy, up_ref), (above, down_copy, down_ref)):
            if there:
                copy(j, d).wait_recv()
                fetch(src.at[j, d], count).start()
                count += 1
        for index in range(count):
            fetch(up_ref.at[j, d], index).wait()
        ref = term_ref(j, d)

        def body(i, carry):
            b, r = strip_of(i)
            value = ref[b, r].astype(F32)
            for index in range(count):
                value += stage[index, b, r].astype(F32)
            value = value.astype(BF16)
            at = pl.ds(pl.multiple_of(i * strip, strip), strip)
            for v in range(K):
                total[j, v, at] = value[:, v * LANES:(v + 1) * LANES]
            return carry

        lax.fori_loop(0, 2 * strips, body, 0)
        for t in range(3):
            fin(j, t, False).start()
        fin_local(j).start()

    for j in range(nj):
        col(j, False).start()
    for h in range(2):
        xy_start(0, h, 0)
        xy_start(0, h, 1)
        xy_start(0, h, 4)

    def col_own(j):
        return pltpu.make_async_copy(
            c_ref.at[x, k, j], cols.at[j, col_rows(z * 2 + x, 1)], own_sem.at[0, j]
        )

    env_own = [
        pltpu.make_async_copy(l_ref.at[h], env.at[y, x, k, h], own_sem.at[1, h]) for h in range(2)
    ]
    conj_own = [
        pltpu.make_async_copy(a_ref.at[h], conj.at[2 * y + h, x], own_sem.at[2, h])
        for h in range(2)
    ]
    for j in range(nj):
        col_own(j).start()
    for copy in env_own + conj_own:
        copy.start()

    for j in range(nj):
        col_own(j).wait()
        col(j, True).wait_recv()
        hop_start(j, 1)
    from_y(0, 0)
    hop_pass(0, 1)
    for j in range(1, nj):
        hop_pass(j, 1)
        if j == 1:
            from_y(0, 1)
            from_x(0, 0)
    from_x(0, 1)
    xy_start(1, 0, 0)
    xy_start(1, 0, 1)
    hop_pass(0, 2)
    diagonal(0, 0)
    diagonal(0, 1)
    for j in range(1, nj):
        hop_pass(j, 2)
    for copy in env_own + conj_own:
        copy.wait()
    from_core(0, 0)
    from_core(0, 1)
    from_y(1, 0)
    from_x(1, 0)
    xy_start(1, 1, 0)
    xy_start(1, 1, 1)

    def product_and_mix(j):
        hop_pass(j, 3)
        first_product(j)
        hop_sent(j)
        mix(j)

    far = (nz - 1, 0)
    near = tuple(d for d in range(nz - 1, -1, -1) if d not in far)
    product_and_mix(0)
    product_and_mix(1)
    diagonal(1, 0)
    from_core(1, 0)
    for j in range(2):
        for d in far:
            second_product(j, d)
    from_y(1, 1)
    from_x(1, 1)
    for j in range(2, nj):
        product_and_mix(j)
    diagonal(1, 1)
    from_core(1, 1)
    for h in range(2):
        for t in range(8):
            xy(0, h, t, False).wait_send()
    for j in range(2):
        for d in near:
            second_product(j, d)
    for j in range(2, nj):
        for d in far + near:
            second_product(j, d)
    order = [(j, d) for j in range(2) for d in far] + [(j, d) for j in range(2) for d in near]
    order += [(j, d) for j in range(2, nj) for d in far + near]
    for own_z in range(nz):
        @pl.when(z == own_z)
        def _():
            for j, d in order:
                d = d if 2 * own_z < nz else nz - 1 - d
                if d == own_z:
                    finish(j, d)
                elif d > own_z and own_z > 0:
                    pass_on(j, d, True)
                elif d < own_z and own_z < nz - 1:
                    pass_on(j, d, False)
            for j, d in order:
                if d > own_z:
                    up_copy(j, d).wait_send()
                elif d < own_z:
                    down_copy(j, d).wait_send()

    for j in range(nj):
        col(j, False).wait_send()
        fin_local(j).wait()
        for t in range(3):
            fin(j, t, False).wait_send()
            fin(j, t, True).wait_recv()
    for h in range(2):
        for t in (0, 1, 2, 3, 5, 6, 7):
            xy(1, h, t, False).wait_send()


def fused(nz, left_env, site_tensor, block_values, pair_in, pair_out):
    rows, phys, width_loc = site_tensor.shape
    nj = width_loc // (4 * LANES)
    mixing = mixing_of(block_values, pair_in, pair_out).reshape(K * phys, K * phys)
    high = lax.reduce_precision(mixing, 8, 7)
    eye = jnp.eye(16, dtype=F32)
    spread = jnp.concatenate([jnp.kron(high, eye), jnp.kron(mixing - high, eye)], axis=0)
    spread = spread.astype(BF16)
    columns = site_tensor.reshape(rows, phys, 2, 2, nj, LANES)
    columns = columns.transpose(2, 3, 4, 0, 1, 5).reshape(2, 2, nj, rows, phys * LANES)
    turned = site_tensor.transpose(2, 1, 0).reshape(2, 2, rows, phys * rows)
    width = phys * LANES
    dma = pltpu.SemaphoreType.DMA
    anywhere = pl.BlockSpec(memory_space=pl.ANY)
    out, _, _ = pl.pallas_call(
        functools.partial(update_kernel, nz, nj, rows, phys),
        out_shape=(
            jax.ShapeDtypeStruct(left_env.shape, BF16),
            jax.ShapeDtypeStruct((nj, nz, 2, rows, width), BF16),
            jax.ShapeDtypeStruct((nj, nz, 2, rows, width), BF16),
        ),
        in_specs=[anywhere, anywhere, anywhere, pl.BlockSpec(memory_space=pltpu.VMEM)],
        out_specs=(anywhere, anywhere, anywhere),
        scratch_shapes=[
            pltpu.VMEM((2, 2, 2, 2, rows, width_loc), BF16),
            pltpu.VMEM((nz, 2, 2, rows, phys * rows), BF16),
            pltpu.VMEM((nj, 2 * nz * rows, width), BF16),
            pltpu.VMEM((2, K, rows, width), BF16),
            pltpu.VMEM((2, nz, 2, rows, width), BF16),
            pltpu.VMEM((2, 2, rows, width), BF16),
            pltpu.VMEM((nj, K, 2 * rows, LANES), BF16),
            dma((3, max(nj, 2))),
            dma((2, 2, 8)), dma((2, 2, 8)),
            dma((nj,)), dma((nj,)),
            dma((nj, 2, nz - 1)), dma((nj, 2, nz - 1)),
            dma((nj, nz)), dma((nj, nz)),
            dma((nj, nz)), dma((nj, nz)),
            dma((2,)),
            dma((nj, 3)), dma((nj, 3)), dma((nj,)),
        ],
        compiler_params=pltpu.CompilerParams(
            collective_id=0, has_side_effects=True, vmem_limit_bytes=67043328
        ),
    )(left_env, turned, columns, spread)
    return out


def solution(mesh):
    sizes = dict(mesh.shape)

    def local(left_env, site_tensor, block_values, pair_in, pair_out):
        comps_loc = left_env.shape[0]
        rows, phys, width = site_tensor.shape
        fits = (
            sizes["ket"] == 2 and sizes["mpo"] == 2 and sizes["bra"] == 8
            and comps_loc == 2 and phys == 4 and rows % 192 == 0
            and width == (sizes["bra"] // 2) * rows and width % (4 * LANES) == 0
            and 2 <= width // (4 * LANES) <= 3 and rows <= 384
        )
        if fits:
            return fused(
                sizes["bra"] // 2, left_env, site_tensor, block_values, pair_in, pair_out
            )
        return plain(left_env, site_tensor, block_values, pair_in, pair_out)

    return jax.shard_map(
        local,
        mesh=mesh,
        in_specs=(P("mpo", "bra", "ket"), P("bra", None, "ket"), P(), P(), P()),
        out_specs=P("mpo", "bra", "ket"),
        check_vma=False,
    )
```

```python
import functools

import jax
import jax.numpy as jnp
from jax import lax
from jax.experimental import pallas as pl
from jax.experimental.pallas import tpu as pltpu
from jax.sharding import PartitionSpec as P

K = 4
LANES = 128
MESH = pl.DeviceIdType.MESH
BF16 = jnp.bfloat16
F32 = jnp.float32


def mixing_of(block_values, pair_in, pair_out):
    comps = jnp.arange(K, dtype=jnp.int32)
    hot_out = (pair_out[:, None] == comps[None, :]).astype(F32)
    hot_in = (pair_in[:, None] == comps[None, :]).astype(F32)
    return jnp.einsum(
        "pv,pw,pst->vswt", hot_out, hot_in, block_values, precision=lax.Precision.HIGHEST
    )


def plain(left_env, site_tensor, block_values, pair_in, pair_out):
    rows_loc = left_env.shape[1]
    cols_loc = left_env.shape[2]
    phys = site_tensor.shape[1]
    mixing = mixing_of(block_values, pair_in, pair_out)
    splits = lax.axis_size("mpo")
    half_cols = cols_loc // splits
    own_start = lax.axis_index("mpo") * half_cols
    site_own = lax.dynamic_slice_in_dim(site_tensor, own_start, half_cols, 2)
    site_full = lax.all_gather(
        site_own.reshape(rows_loc, phys * half_cols), "bra", axis=0, tiled=True
    )
    piece = lax.all_gather(left_env, "ket", axis=2, tiled=True)
    piece = lax.all_gather(piece, "mpo", axis=0, tiled=True)
    comps_all, width = piece.shape[0], piece.shape[2]
    half = jnp.dot(
        piece.reshape(comps_all * rows_loc, width), site_full, preferred_element_type=F32
    )
    half = half.astype(BF16).reshape(comps_all, rows_loc, phys, half_cols)
    mixed = jnp.einsum(
        "vswt,watc->savc", mixing, half.astype(F32), precision=lax.Precision.HIGHEST
    ).astype(BF16)
    mixed_pairs = mixed.reshape(phys * rows_loc, comps_all * half_cols)
    site_wide = lax.all_gather(
        jnp.transpose(site_tensor, (1, 0, 2)), "ket", axis=2, tiled=True
    )
    site_pairs = site_wide.reshape(phys * rows_loc, site_wide.shape[2])
    term = lax.dot_general(
        site_pairs, mixed_pairs, (((0,), (0,)), ((), ())), preferred_element_type=F32
    ).astype(BF16)
    owned = lax.psum_scatter(term, "bra", scatter_dimension=0, tiled=True)
    owned = jnp.transpose(owned.reshape(-1, comps_all, half_cols), (1, 0, 2))
    return lax.all_to_all(owned, "mpo", split_axis=0, concat_axis=2, tiled=True)


def update_kernel(
    nz, nj, rows, phys,
    l_ref, s_ref, mix_ref,
    out_ref, up_ref, down_ref,
    env, conj, cols, half, terms, stage, raw, spread,
    own_sem, raw_sem, xy_send, xy_recv, col_send, col_recv, z_send, z_recv,
    up_send, up_recv, down_send, down_recv, stage_sem, fin_send, fin_recv, fin_own,
):
    bra, y, k = lax.axis_index("bra"), lax.axis_index("ket"), lax.axis_index("mpo")
    z, x = bra // 2, lax.rem(bra, 2)
    xo, yo, ko = 1 - x, 1 - y, 1 - k
    xn, yn, kn = (z * 2 + xo, y, k), (bra, yo, k), (bra, y, ko)
    xkn = (z * 2 + xo, y, ko)
    zu, zd = (bra + 2, y, k), (bra - 2, y, k)
    has_up, has_down = z < nz - 1, z > 0
    width = phys * LANES
    part = rows // 2

    barrier = pltpu.get_barrier_semaphore()
    for device in (xn, yn, kn, xkn):
        pl.semaphore_signal(barrier, inc=1, device_id=device, device_id_type=MESH)

    @pl.when(has_up)
    def _():
        pl.semaphore_signal(barrier, inc=1, device_id=zu, device_id_type=MESH)

    @pl.when(has_down)
    def _():
        pl.semaphore_signal(barrier, inc=1, device_id=zd, device_id_type=MESH)

    pl.semaphore_wait(barrier, 4 + (z + nz - 1) // nz + (2 * nz - 2 - z) // nz)

    def remote(src, dst, send, recv, device):
        return pltpu.make_async_remote_copy(
            src_ref=src, dst_ref=dst, send_sem=send, recv_sem=recv,
            device_id=device, device_id_type=MESH,
        )

    def slot(q, xs, ys, ks, h):
        if q == 0:
            return env.at[ys, xs, ks, h]
        return conj.at[2 * ys + lax.rem(h // 2 + ys, 2), xs, ks, pl.ds(h % 2 * part, part)]

    def own(q, h):
        return l_ref.at[h] if q == 0 else slot(1, x, y, k, h)

    def whole_over_y(q, h):
        return q == 0 and h == 0

    def xy(q, h, t, receiving):
        ks = ko if receiving else k
        size = part if q == 0 else part // 2
        upper, lower = pl.ds(0, size), pl.ds(size, size)
        if t == 0:
            dst = slot(q, xo if receiving else x, y, k, h)
            src, device = own(q, h), xn
        elif t == 1:
            dst = slot(q, x, yo if receiving else y, k, h)
            src, device = own(q, h), yn
        elif t == 2:
            dst = slot(q, xo if receiving else x, yo, k, h).at[lower]
            src, device = dst, xn
        elif t == 3:
            dst = slot(q, xo, yo if receiving else y, k, h)
            dst = dst if whole_over_y(q, h) else dst.at[upper]
            src, device = dst, yn
        else:
            dst = slot(q, xo if t in (5, 7) else x, yo if t in (6, 7) else y, ks, h)
            src, device = own(q, h) if t == 4 else dst, kn
        if receiving:
            src = dst
        return remote(src, dst, xy_send.at[q, h, t], xy_recv.at[q, h, t], device)

    def xy_start(q, h, t):
        xy(q, h, t, False).start()

    def xy_wait(q, h, t):
        xy(q, h, t, True).wait_recv()

    def from_x(q, h):
        xy_wait(q, h, 0)
        xy_start(q, h, 3)
        xy_start(q, h, 5)

    def from_y(q, h):
        xy_wait(q, h, 1)
        if not whole_over_y(q, h):
            xy_start(q, h, 2)
        xy_start(q, h, 6)

    def diagonal(q, h):
        if not whole_over_y(q, h):
            xy_wait(q, h, 2)
        xy_wait(q, h, 3)
        xy_start(q, h, 7)

    def from_core(q, h):
        for t in range(4 if q == 0 else 5, 8):
            xy_wait(q, h, t)

    def col_rows(index, count):
        return pl.ds(pl.multiple_of(index * rows, rows), count * rows)

    def col(j, receiving):
        dst = cols.at[j, col_rows(z * 2 + (xo if receiving else x), 1)]
        return remote(half.at[1, j], dst, col_send.at[j], col_recv.at[j], xn)

    def hop(j, up, s, receiving):
        piece = (z - s if receiving else z - s + 1) if up else (z + s if receiving else z + s - 1)
        ref = cols.at[j, col_rows(piece * 2, 2)]
        way = 0 if up else 1
        return remote(
            ref, ref, z_send.at[j, way, s - 1], z_recv.at[j, way, s - 1], zu if up else zd
        )

    def hop_sends(up, s):
        return (has_up & (z >= s - 1)) if up else (has_down & (z <= nz - s))

    def hop_start(j, s):
        for up in (True, False):
            @pl.when(hop_sends(up, s))
            def _():
                hop(j, up, s, False).start()

    def hop_sent(j):
        for s in range(1, nz):
            for up in (True, False):
                @pl.when(hop_sends(up, s))
                def _():
                    hop(j, up, s, False).wait_send()

    def hop_pass(j, s):
        for up in (True, False):
            @pl.when((z >= s) if up else (z < nz - s))
            def _():
                hop(j, up, s, True).wait_recv()

            if s < nz - 1:
                @pl.when(hop_sends(up, s + 1))
                def _():
                    hop(j, up, s + 1, False).start()

    deep = nz * rows

    def first_product(j, begin=0, end=4):
        def body(i, carry):
            xs, ks = i // 2, lax.rem(i, 2)
            acc = jnp.dot(
                env[0, xs, ks].reshape(2 * rows, deep), cols[j, :deep], preferred_element_type=F32
            )
            acc += jnp.dot(
                env[1, xs, ks].reshape(2 * rows, deep), cols[j, deep:], preferred_element_type=F32
            )
            half[xs, pl.ds(2 * ks, 2)] = acc.astype(BF16).reshape(2, rows, width)
            return carry

        lax.fori_loop(begin, end, body, 0)

    group = 4
    span = group * 16

    def mix(j):
        per_x = rows // span

        def body(i, carry):
            xs, base = i // per_x, pl.multiple_of(lax.rem(i, per_x) * span, span)
            tiles = [
                half[xs, w, pl.ds(base, span), t * LANES:(t + 1) * LANES]
                for w in range(K) for t in range(phys)
            ]
            right = jnp.concatenate(
                [
                    jnp.concatenate([tile[g * 16:(g + 1) * 16] for tile in tiles], axis=0)
                    for g in range(group)
                ],
                axis=1,
            )
            both = jnp.dot(spread[...], right, preferred_element_type=F32)
            size = K * phys * 16
            result = (both[:size] + both[size:]).astype(BF16)
            size = 16 * phys
            for v in range(K):
                for g in range(group):
                    at = pl.multiple_of(xs * deep + (base + g * 16) * phys, size)
                    cols[j, pl.ds(at, size), v * LANES:(v + 1) * LANES] = result[
                        v * size:(v + 1) * size, g * LANES:(g + 1) * LANES
                    ]
            return carry

        lax.fori_loop(0, 2 * per_x, body, 0)

    def term_ref(j, d, g):
        at = pl.ds(g * part, part)
        if j < 2:
            return terms.at[j, d, :, at]
        return env.at[d // 2, lax.rem(d, 2), 0, :, at, pl.ds((j - 2) * width, width)]

    def up_copy(j, d, g):
        return remote(
            term_ref(j, d, g), up_ref.at[j, d, :, pl.ds(g * part, part)],
            up_send.at[j, d, g], up_recv.at[j, d, g], zu,
        )

    def down_copy(j, d, g):
        return remote(
            term_ref(j, d, g), down_ref.at[j, d, :, pl.ds(g * part, part)],
            down_send.at[j, d, g], down_recv.at[j, d, g], zd,
        )

    def second_product(j, d, g, ups=True, downs=True):
        out = term_ref(j, d, g)
        at = slice(g * part, (g + 1) * part)
        acc = jnp.dot(
            conj[d, 0, :, at].reshape(rows, deep), cols[j, :deep], preferred_element_type=F32
        )
        acc += jnp.dot(
            conj[d, 1, :, at].reshape(rows, deep), cols[j, deep:], preferred_element_type=F32
        )
        out[...] = acc.astype(BF16).reshape(2, part, width)
        if ups:
            @pl.when(z == 0)
            def _():
                up_copy(j, d, g).start()
        if downs:
            @pl.when(z == nz - 1)
            def _():
                down_copy(j, d, g).start()

    def far_products(j, g):
        second_product(j, nz - 1, g, downs=False)
        second_product(j, 0, g, ups=False)

    strip = part // 2
    strips = part // strip

    def strip_of(i):
        return i // strips, pl.ds(pl.multiple_of(lax.rem(i, strips) * strip, strip), strip)

    def fetch(src, index):
        return pltpu.make_async_copy(src, stage.at[index], stage_sem.at[index])

    def landed(ref, j, d, g):
        return ref.at[j, d, :, pl.ds(g * part, part)]

    def pass_on(j, d, g, up):
        copy = up_copy(j, d, g) if up else down_copy(j, d, g)
        copy.wait_recv()
        local = fetch(landed(up_ref if up else down_ref, j, d, g), 0)
        local.start()
        local.wait()
        ref = term_ref(j, d, g)

        def body(i, carry):
            b, r = strip_of(i)
            ref[b, r] = (ref[b, r].astype(F32) + stage[0, b, r].astype(F32)).astype(BF16)
            return carry

        lax.fori_loop(0, 2 * strips, body, 0)
        copy.start()

    def place(block, j, g):
        at = pl.multiple_of((block * nj + j) * LANES, LANES)
        return out_ref.at[:, pl.ds(g * part, part), pl.ds(at, LANES)]

    def summed(xs, ks, j, g):
        at = slice(j * LANES, (j + 1) * LANES)
        return half.at[xs, pl.ds(2 * ks, 2), pl.ds(g * part, part), at]

    def fin(j, g, t, receiving):
        xs, ks, device = ((x, ko, kn), (xo, k, xn), (xo, ko, xkn))[t]
        dst = place((xs * 2 + ks) if receiving else (x * 2 + k), j, g)
        return remote(
            summed(xs, ks, j, g), dst, fin_send.at[j, g, t], fin_recv.at[j, g, t], device
        )

    def fin_local(j, g):
        return pltpu.make_async_copy(
            summed(x, k, j, g), place(x * 2 + k, j, g), fin_own.at[j, g]
        )

    def finish(j, d, g):
        below, above = d > 0, d < nz - 1
        count = 0
        for there, copy, src in ((below, up_copy, up_ref), (above, down_copy, down_ref)):
            if there:
                copy(j, d, g).wait_recv()
                fetch(landed(src, j, d, g), count).start()
                count += 1
        for index in range(count):
            fetch(landed(up_ref, j, d, g), index).wait()
        ref = term_ref(j, d, g)

        def body(i, carry):
            b, r = strip_of(i)
            value = ref[b, r].astype(F32)
            for index in range(count):
                value += stage[index, b, r].astype(F32)
            value = value.astype(BF16)
            at = pl.ds(pl.multiple_of(g * part + lax.rem(i, strips) * strip, strip), strip)
            for v in range(K):
                half[b, v, at, j * LANES:(j + 1) * LANES] = value[:, v * LANES:(v + 1) * LANES]
            return carry

        lax.fori_loop(0, 2 * strips, body, 0)
        for t in (1, 2, 0):
            fin(j, g, t, False).start()
        fin_local(j, g).start()

    deal = 64
    deals = rows // deal
    lump = deal * phys

    def load(i):
        at = pl.ds(i * deal, deal)
        return pltpu.make_async_copy(s_ref.at[at], raw.at[i % 2], raw_sem.at[i % 2])

    def each_deal(work):
        load(0).start()
        for i in range(deals):
            if i + 1 < deals:
                load(i + 1).start()
            load(i).wait()
            work(i)

    row_id = lax.broadcasted_iota(jnp.int32, (lump, lump), 0)
    col_id = lax.broadcasted_iota(jnp.int32, (lump, lump), 1)
    wanted = (row_id & (deal - 1)) * phys + row_id // deal
    permute = (col_id == wanted).astype(F32).astype(BF16)

    def to_cols(i):
        for xs in (xo, x):
            at = pl.ds(pl.multiple_of((xs * 2 + k) * nj * LANES, LANES), nj * LANES)
            piece = raw[i % 2, :, :, at].reshape(lump, nj * LANES)
            piece = jnp.dot(permute, piece, preferred_element_type=F32).astype(BF16)
            for j in range(nj):
                for t in range(phys):
                    tile = piece[t * deal:(t + 1) * deal, j * LANES:(j + 1) * LANES]
                    lanes = slice(t * LANES, (t + 1) * LANES)
                    if xs is xo:
                        half[1, j, i * deal:(i + 1) * deal, lanes] = tile
                    else:
                        base = pl.multiple_of((z * 2 + x) * rows + i * deal, deal)
                        cols[j, pl.ds(base, deal), lanes] = tile

    def to_conj(i):
        for dl in range(2):
            for kk in range(2):
                at = (dl * 2 + kk) * rows
                piece = raw[i % 2, :, :, at:at + rows].reshape(lump, rows)
                conj[2 * y + dl, x, kk, :, i * lump:(i + 1) * lump] = piece.T

    def make_spread():
        pairs, size = K * phys, K * phys * 16
        ids = lambda shape, dim: lax.broadcasted_iota(jnp.int32, shape, dim)
        one_hot = lambda match: match.astype(F32).astype(BF16)
        out, kind = ids((size, pairs), 0), ids((size, pairs), 1)
        left = one_hot(out // (16 * phys) * phys + (out & (phys - 1)) == kind)
        kind, into = ids((pairs, size), 0), ids((pairs, size), 1)
        right = one_hot(into // 16 == kind)
        out, into = ids((size, size), 0), ids((size, size), 1)
        same = ((out // phys) & 15) == (into & 15)
        high = mix_ref[...].astype(BF16)
        low = (mix_ref[...] - high.astype(F32)).astype(BF16)
        for index, value in enumerate((high, low)):
            rows_of = jnp.dot(left, value, preferred_element_type=F32).astype(BF16)
            full = jnp.dot(rows_of, right, preferred_element_type=F32)
            full = jnp.where(same, full, 0.0).astype(BF16)
            spread[index * size:(index + 1) * size] = full

    for h in range(2):
        xy_start(0, h, 1)
        xy_start(0, h, 4)
    env_own = [
        pltpu.make_async_copy(l_ref.at[h], env.at[y, x, k, h], own_sem.at[h]) for h in range(2)
    ]
    each_deal(to_cols)
    for j in range(nj):
        col(j, False).start()
    for h in range(2):
        xy_start(0, h, 0)
    for copy in env_own:
        copy.start()
    each_deal(to_conj)
    make_spread()

    def hop_first(j):
        col(j, True).wait_recv()
        hop_start(j, 1)

    hop_first(0)
    from_y(0, 0)
    hop_pass(0, 1)
    from_y(0, 1)
    hop_pass(0, 2)
    hop_first(1)
    from_x(0, 0)
    hop_pass(0, 3)
    hop_pass(1, 1)
    from_x(0, 1)
    xy_start(1, 0, 0)
    xy_start(1, 0, 1)
    hop_pass(1, 2)
    for j in range(2, nj):
        hop_first(j)
    diagonal(0, 0)
    diagonal(0, 1)
    for copy in env_own:
        copy.wait()
    for j in range(nj):
        col(j, False).wait_send()
    from_core(0, 0)
    from_core(0, 1)

    waiting = [[] for _ in range(nz)]

    def reduce(order, last=False):
        for own_z in range(nz):
            tasks = []
            for j, d, g in order:
                d = d if 2 * own_z < nz else nz - 1 - d
                if d == own_z and not last:
                    waiting[own_z].append((j, d, g))
                else:
                    tasks.append((j, d, g))
            if last:
                tasks = waiting[own_z] + tasks

            @pl.when(z == own_z)
            def _():
                for j, d, g in tasks:
                    if d == own_z:
                        finish(j, d, g)
                    elif d > own_z and own_z > 0:
                        pass_on(j, d, g, True)
                    elif d < own_z and own_z < nz - 1:
                        pass_on(j, d, g, False)

    second = nz - 2 - z // 2
    third = 1 + z // 2
    late = range(2, nj)

    first_product(0, 0, 2)
    from_y(1, 0)
    from_x(1, 0)
    for h in (1, 2):
        xy_start(1, h, 0)
        xy_start(1, h, 1)
    first_product(0, 2, 4)
    hop_sent(0)
    mix(0)
    diagonal(1, 0)
    from_core(1, 0)
    far_products(0, 0)
    hop_pass(1, 3)
    first_product(1, 0, 2)
    from_y(1, 1)
    from_x(1, 1)
    xy_start(1, 3, 0)
    xy_start(1, 3, 1)
    first_product(1, 2, 4)
    hop_sent(1)
    mix(1)
    far_products(1, 0)
    for j in late:
        hop_pass(j, 1)
    reduce([(0, 3, 0)])
    diagonal(1, 1)
    from_core(1, 1)
    far_products(0, 1)
    far_products(1, 1)
    from_y(1, 2)
    from_x(1, 2)
    for j in late:
        hop_pass(j, 2)
    reduce([(1, 3, 0)])
    from_y(1, 3)
    from_x(1, 3)
    diagonal(1, 2)
    from_core(1, 2)
    second_product(0, second, 0)
    second_product(1, second, 0)
    reduce([(0, 3, 1), (1, 3, 1)])
    diagonal(1, 3)
    from_core(1, 3)
    second_product(0, second, 1)
    second_product(1, second, 1)
    reduce([(0, 0, 0), (1, 0, 0), (0, 2, 0)])
    for j in late:
        hop_pass(j, 3)
        first_product(j)
        hop_sent(j)
        mix(j)
    for h in range(2):
        for t in range(8):
            if t != 2 or not whole_over_y(0, h):
                xy(0, h, t, False).wait_send()
    for j in late:
        for g in range(2):
            far_products(j, g)
    reduce([(1, 2, 0), (0, 0, 1), (1, 0, 1), (0, 2, 1)])
    for j in late:
        for g in range(2):
            second_product(j, second, g)
    for j in range(nj):
        for g in range(2):
            second_product(j, third, g)
    rest = [(1, 2, 1)]
    for j in late:
        rest += [(j, 3, 0), (j, 3, 1), (j, 2, 0), (j, 0, 0), (j, 2, 1), (j, 0, 1)]
    reduce(rest + [(j, 1, g) for j in range(nj) for g in range(2)], last=True)
    for own_z in range(nz):
        @pl.when(z == own_z)
        def _():
            for j in range(nj):
                for g in range(2):
                    for d in range(nz):
                        if d > own_z:
                            up_copy(j, d, g).wait_send()
                        elif d < own_z:
                            down_copy(j, d, g).wait_send()

    for j in range(nj):
        for g in range(2):
            fin_local(j, g).wait()
            for t in range(3):
                fin(j, g, t, False).wait_send()
                fin(j, g, t, True).wait_recv()
    for h in range(4):
        for t in (0, 1, 2, 3, 5, 6, 7):
            xy(1, h, t, False).wait_send()


def fused(nz, left_env, site_tensor, block_values, pair_in, pair_out):
    rows, phys, width_loc = site_tensor.shape
    nj = width_loc // (4 * LANES)
    mixing = mixing_of(block_values, pair_in, pair_out).reshape(K * phys, K * phys)
    width = phys * LANES
    dma = pltpu.SemaphoreType.DMA
    anywhere = pl.BlockSpec(memory_space=pl.ANY)
    out, _, _ = pl.pallas_call(
        functools.partial(update_kernel, nz, nj, rows, phys),
        out_shape=(
            jax.ShapeDtypeStruct(left_env.shape, BF16),
            jax.ShapeDtypeStruct((nj, nz, 2, rows, width), BF16),
            jax.ShapeDtypeStruct((nj, nz, 2, rows, width), BF16),
        ),
        in_specs=[anywhere, anywhere, pl.BlockSpec(memory_space=pltpu.VMEM)],
        out_specs=(anywhere, anywhere, anywhere),
        scratch_shapes=[
            pltpu.VMEM((2, 2, 2, 2, rows, width_loc), BF16),
            pltpu.VMEM((nz, 2, 2, rows, rows * phys), BF16),
            pltpu.VMEM((nj, 2 * nz * rows, width), BF16),
            pltpu.VMEM((2, K, rows, width), BF16),
            pltpu.VMEM((2, nz, 2, rows, width), BF16),
            pltpu.VMEM((2, 2, rows // 2, width), BF16),
            pltpu.VMEM((2, 64, phys, width_loc), BF16),
            pltpu.VMEM((2 * K * phys * 16, K * phys * 16), BF16),
            dma((2,)), dma((2,)),
            dma((2, 4, 8)), dma((2, 4, 8)),
            dma((nj,)), dma((nj,)),
            dma((nj, 2, nz - 1)), dma((nj, 2, nz - 1)),
            dma((nj, nz, 2)), dma((nj, nz, 2)),
            dma((nj, nz, 2)), dma((nj, nz, 2)),
            dma((2,)),
            dma((nj, 2, 3)), dma((nj, 2, 3)), dma((nj, 2)),
        ],
        compiler_params=pltpu.CompilerParams(
            collective_id=0, has_side_effects=True, vmem_limit_bytes=67043328
        ),
    )(left_env, site_tensor, mixing)
    return out


def solution(mesh):
    sizes = dict(mesh.shape)

    def local(left_env, site_tensor, block_values, pair_in, pair_out):
        comps_loc = left_env.shape[0]
        rows, phys, width = site_tensor.shape
        fits = (
            sizes["ket"] == 2 and sizes["mpo"] == 2 and sizes["bra"] == 8
            and comps_loc == 2 and phys == 4 and rows % 192 == 0
            and width == (sizes["bra"] // 2) * rows and width % (4 * LANES) == 0
            and 2 <= width // (4 * LANES) <= 3 and rows <= 384
        )
        if fits:
            return fused(
                sizes["bra"] // 2, left_env, site_tensor, block_values, pair_in, pair_out
            )
        return plain(left_env, site_tensor, block_values, pair_in, pair_out)

    return jax.shard_map(
        local,
        mesh=mesh,
        in_specs=(P("mpo", "bra", "ket"), P("bra", None, "ket"), P(), P(), P()),
        out_specs=P("mpo", "bra", "ket"),
        check_vma=False,
    )
```
